32 devices in a mesh: grp: 2 (over y), seq: 4 (over z), head: 4 (over x, core).
Axes of the slice: x: 2, y: 2, z: 4, core: 2. Of those that a mesh axis runs over, the one named last changes fastest.
Arguments:
- queries: bfloat16 [1024, 32, 128], P(('grp', 'seq'), 'head'), parts along dimension 0, may hold values from -26 to 26
- keys: bfloat16 [1024, 8, 128], P(('grp', 'seq'), 'head'), parts along dimension 0, may hold values from -13 to 13
- values: bfloat16 [1024, 8, 128], P(('grp', 'seq'), 'head'), parts along dimension 0, may hold values from -6 to 6
- block_order: int32 [16], P('grp'), parts along dimension 0, may hold values from 0 to 7, as said below
Outputs:
- attended: bfloat16 [1024, 32, 128], P(('grp', 'seq'), 'head'), parts along dimension 0
The draws below stay inside these ranges and needn't reach their ends.
There are 2 independent parts, one for each index of `grp`. The reference program is written for one: setup_inputs(seed, part) draws one part's arguments, and reference() takes and returns one part's arrays. A program takes and returns all parts, laid end to end along the dimension named above; each array names one. Nothing has to cross between parts.
Inputs may be any that keep to these rules, and one draw needn't show every extreme that they name: `block_order`: slots 2 i and 2 i + 1 hold blocks c and 7 - c for some c, in either order; every block stands in one slot.
All inputs are finite; a program needn't handle non-finite values.
Results may differ from the reference program's by a relative error of at most 0.0055.
Values may be sent and summed in bfloat16 or wider, within the bound.
A program may use at most 128 MiB of HBM per device.

```python
import jax
import jax.numpy as jnp
from jax import lax

QH = 32
KVH = 8
HD = 128
TOK_DEV = 128
BLOCK = 64
TOKENS = 512
N_SEQ = 4


def pair_order(key):
    count = N_SEQ
    shuffled = jax.random.permutation(jax.random.fold_in(key, 11), count).astype(jnp.int32)
    flips = jax.random.randint(jax.random.fold_in(key, 12), (count,), 0, 2).astype(jnp.int32)
    first = jnp.where(flips == 0, shuffled, 2 * count - 1 - shuffled)
    second = 2 * count - 1 - first
    return jnp.stack([first, second], axis=1).reshape(2 * count).astype(jnp.int32)


def draw_block_order(key, part):
    return pair_order(key)


def draw_queries(key, part):
    base = jnp.clip(jax.random.normal(jax.random.fold_in(key, 21), (TOKENS, QH, HD), jnp.float32), -5.0, 5.0)
    return base.astype(jnp.bfloat16)


def draw_keys(key, part):
    base = jnp.clip(jax.random.normal(jax.random.fold_in(key, 22), (TOKENS, KVH, HD), jnp.float32), -5.0, 5.0)
    return base.astype(jnp.bfloat16)


def levels(stream_key, shape, cuts, smallest, largest):
    gain = 1.0
    for position, parts in cuts:
        steps = jax.random.uniform(jax.random.fold_in(jax.random.fold_in(stream_key, 6), position), (parts,), jnp.float32, smallest / len(cuts), largest / len(cuts))
        gain = gain * jnp.repeat(jnp.exp(steps), shape[position] // parts).reshape((-1,) + (1,) * (len(shape) - 1 - position))
    return gain


def normal_values(own_key, shape, spread, most, pieces=(), kind=jnp.bfloat16):
    factor_of = levels(own_key, shape, pieces, -0.22, 0.18) if pieces else 1.0
    values = jax.random.normal(own_key, shape, jnp.float32) * spread * factor_of
    return jnp.minimum(jnp.maximum(values, -most), most).astype(kind)


def setup_inputs(seed: int = 0, part: int = 0) -> dict:
    arg_keys = jax.random.split(jax.random.key(seed), 5)
    part_splits = jax.random.split(jax.random.fold_in(arg_keys[4], part), 5)
    return {
        "queries": draw_queries(jax.random.fold_in(jax.random.fold_in(arg_keys[4], part), 71), part),
        "keys": draw_keys(jax.random.fold_in(jax.random.fold_in(arg_keys[4], part), 71), part),
        "values": normal_values(part_splits[2], (TOKENS, KVH, HD), 1.0, 6.0, ((0, 4), (1, 4))),
        "block_order": draw_block_order(jax.random.fold_in(jax.random.fold_in(arg_keys[4], part), 71), part),
    }


def reference(queries, keys, values, block_order):
    rows = jnp.arange(TOKENS, dtype=jnp.int32)
    positions = block_order[rows // BLOCK].astype(jnp.int32) * BLOCK + rows % BLOCK
    key_float = keys.astype(jnp.float32)
    value_float = values.astype(jnp.float32)
    group_size = QH // KVH
    score_scale = HD ** -0.5

    def one_block(index):
        start = (index * TOK_DEV).astype(jnp.int32)
        query_rows = lax.dynamic_slice_in_dim(queries, start, TOK_DEV, 0).astype(jnp.float32)
        query_rows = query_rows.reshape(TOK_DEV, KVH, group_size, HD)
        query_pos = lax.dynamic_slice_in_dim(positions, start, TOK_DEV, 0)
        scores = jnp.einsum("cghd,pgd->ghcp", query_rows, key_float) * score_scale
        visible = (positions[None, :] <= query_pos[:, None])[None, None]
        top = jnp.max(jnp.where(visible, scores, -1e30), axis=-1)
        weights = jnp.where(visible, jnp.exp(scores - top[..., None]), 0.0)
        total = jnp.sum(weights, axis=-1)
        rounded = lax.optimization_barrier(weights.astype(jnp.bfloat16)).astype(jnp.float32)
        summed = jnp.einsum("ghcp,pgd->ghcd", rounded, value_float)
        result = summed / total[..., None]
        return jnp.transpose(result, (2, 0, 1, 3)).reshape(TOK_DEV, QH, HD).astype(jnp.bfloat16)

    blocks = lax.map(one_block, jnp.arange(N_SEQ, dtype=jnp.int32))
    return blocks.reshape(TOKENS, QH, HD)
```

```python
import functools
import math

import jax
import jax.numpy as jnp
from jax import lax
from jax.experimental import pallas as pl
from jax.experimental.pallas import tpu as pltpu
from jax.sharding import PartitionSpec as P

MESH = pl.DeviceIdType.MESH
NEG = -1e30


def gather_attend(
    n,
    heads,
    groups,
    tile,
    table_ref,
    q_hbm,
    k_hbm,
    v_hbm,
    out_ref,
    q_ref,
    kv_ref,
    p_ref,
    m_ref,
    l_ref,
    acc_ref,
    load_sem,
    send_sem,
    recv_sem,
):
    me = lax.axis_index("seq")
    rows, width = q_ref.shape
    tokens = rows // heads
    half = tokens // 2
    per_group = heads // groups
    cols = tokens * groups
    piece = cols // 2
    factor_scale = width ** (-0.5) * math.log2(math.e)
    right, left = me + 1, me - 1
    has_right, has_left = me < n - 1, me > 0
    interior = jnp.logical_and(has_right, has_left)

    loads = [
        pltpu.make_async_copy(k_hbm, kv_ref.at[me, 0], load_sem.at[0]),
        pltpu.make_async_copy(v_hbm, kv_ref.at[me, 1], load_sem.at[1]),
        pltpu.make_async_copy(q_hbm, q_ref, load_sem.at[2]),
    ]
    for load in loads:
        load.start()

    barrier = pltpu.get_barrier_semaphore()

    @pl.when(has_right)
    def _():
        pl.semaphore_signal(barrier, inc=1, device_id={"seq": right}, device_id_type=MESH)

    @pl.when(has_left)
    def _():
        pl.semaphore_signal(barrier, inc=1, device_id={"seq": left}, device_id_type=MESH)

    pl.semaphore_wait(barrier, has_right.astype(jnp.int32) + has_left.astype(jnp.int32))

    def part(shard, which):
        return kv_ref.at[shard, which // 2, pl.ds((which % 2) * piece, piece)]

    def remote(shard, which, way, target):
        return pltpu.make_async_remote_copy(
            src_ref=part(shard, which),
            dst_ref=part(shard, which),
            send_sem=send_sem.at[way, shard, which],
            recv_sem=recv_sem.at[shard, which],
            device_id={"seq": target},
            device_id_type=MESH,
        )

    for kind in range(2):
        loads[kind].wait()
        for which in (2 * kind, 2 * kind + 1):

            @pl.when(has_right)
            def _():
                remote(me, which, 0, right).start()

            @pl.when(has_left)
            def _():
                remote(me, which, 1, left).start()

    m_ref[...] = jnp.full(m_ref.shape, NEG, jnp.float32)
    l_ref[...] = jnp.zeros(l_ref.shape, jnp.float32)
    acc_ref[...] = jnp.zeros(acc_ref.shape, jnp.float32)
    loads[2].wait()

    paired = jnp.minimum(me, n - 1 - me)

    def arrival(step):
        near = (step + 1) // 2
        both = jnp.where(step % 2 == 1, me - near, me + near)
        one = jnp.where(me < n - 1 - me, me + step - paired, me - step + paired)
        return jnp.where(step <= 2 * paired, both, one)

    def route(shard):
        from_left = shard < me
        way = jnp.where(from_left, 0, 1)
        return way, jnp.where(from_left, right, left)

    lane = lax.broadcasted_iota(jnp.int32, (heads, cols), 1)
    head = lax.broadcasted_iota(jnp.int32, (heads, cols), 0)
    matched = lane % groups == head // per_group
    key_token = lane // groups

    def receive(shard, which):
        remote(shard, which, 0, me).wait_recv()

    def pass_on(shard, which):
        way, target = route(shard)

        @pl.when(interior)
        def _():
            remote(shard, which, way, target).start()

    def scores(shard):
        first, second = table_ref[2 * shard], table_ref[2 * shard + 1]
        key_pos = jnp.where(
            key_token < half, first * half + key_token, (second - 1) * half + key_token
        )
        key_code = jnp.where(matched, key_pos, 2**30)
        key_rows = kv_ref[shard, 0]
        for start in range(0, tokens, tile):
            span = pl.ds(start * heads, tile * heads)
            block = table_ref[2 * me + start // half]
            offset = block * half + start % half
            raw = lax.dot_general(
                q_ref[span, :],
                key_rows,
                (((1,), (1,)), ((), ())),
                preferred_element_type=jnp.float32,
            )
            shaped = raw.reshape(tile, heads, cols)
            query_pos = lax.broadcasted_iota(jnp.int32, shaped.shape, 0) + offset
            shaped = jnp.where(key_code[None] <= query_pos, shaped, NEG)
            raw = shaped.reshape(tile * heads, cols)
            old_max = m_ref[span, :]
            new_max = jnp.maximum(old_max, jnp.max(raw, axis=-1, keepdims=True))
            fade = jnp.exp2((old_max - new_max) * factor_scale)
            total = l_ref[span, :] * fade
            for low in range(0, cols, width):
                weights = jnp.exp2((raw[:, low : low + width] - new_max) * factor_scale)
                total += weights
                p_ref[span, low : low + width] = weights.astype(p_ref.dtype)
            m_ref[span, :] = new_max
            l_ref[span, :] = total
            acc_ref[span, :] = acc_ref[span, :] * fade

    def weigh(shard):
        value_rows = kv_ref[shard, 1]
        for start in range(0, tokens, tile):
            span = pl.ds(start * heads, tile * heads)
            acc_ref[span, :] += jnp.dot(
                p_ref[span, :], value_rows, preferred_element_type=jnp.float32
            )

    def step(index, carry):
        shard = arrival(index)
        received = index > 0

        @pl.when(received)
        def _():
            for which in (0, 1):
                receive(shard, which)
                pass_on(shard, which)

        @pl.when(jnp.logical_and(received, interior))
        def _():
            for which in (2, 3):
                receive(shard, which)
                pass_on(shard, which)

        scores(shard)

        @pl.when(jnp.logical_and(received, jnp.logical_not(interior)))
        def _():
            for which in (2, 3):
                receive(shard, which)

        weigh(shard)
        return carry

    lax.fori_loop(0, n, step, 0)

    for start in range(0, tokens, tile):
        span = pl.ds(start * heads, tile * heads)
        total = jnp.sum(l_ref[span, :], axis=-1, keepdims=True)
        out_ref[span, :] = (acc_ref[span, :] / total).astype(out_ref.dtype)

    def settle(index, carry):
        shard = arrival(index)

        @pl.when(interior)
        def _():
            way, target = route(shard)
            for which in range(4):
                remote(shard, which, way, target).wait_send()

        return carry

    for which in range(4):

        @pl.when(has_right)
        def _():
            remote(me, which, 0, right).wait_send()

        @pl.when(has_left)
        def _():
            remote(me, which, 1, left).wait_send()

    lax.fori_loop(1, n, settle, 0)


def on_device(queries, keys, values, block_order):
    n = lax.axis_size("seq")
    tokens, heads, width = queries.shape
    groups = keys.shape[1]
    rows, cols = tokens * heads, tokens * groups
    tile = min(32, tokens // 2)
    anywhere = pl.BlockSpec(memory_space=pl.ANY)
    out = pl.pallas_call(
        functools.partial(gather_attend, n, heads, groups, tile),
        out_shape=jax.ShapeDtypeStruct((rows, width), queries.dtype),
        in_specs=[pl.BlockSpec(memory_space=pltpu.SMEM), anywhere, anywhere, anywhere],
        out_specs=pl.BlockSpec(memory_space=pltpu.VMEM),
        scratch_shapes=[
            pltpu.VMEM((rows, width), queries.dtype),
            pltpu.VMEM((n, 2, cols, width), keys.dtype),
            pltpu.VMEM((rows, cols), values.dtype),
            pltpu.VMEM((rows, width), jnp.float32),
            pltpu.VMEM((rows, width), jnp.float32),
            pltpu.VMEM((rows, width), jnp.float32),
            pltpu.SemaphoreType.DMA((3,)),
            pltpu.SemaphoreType.DMA((2, n, 4)),
            pltpu.SemaphoreType.DMA((n, 4)),
        ],
        compiler_params=pltpu.CompilerParams(collective_id=0, has_side_effects=True),
    )(
        block_order,
        queries.reshape(rows, width),
        keys.reshape(cols, width),
        values.reshape(cols, width),
    )
    return out.reshape(tokens, heads, width)


def solution(mesh):
    placed = P(("grp", "seq"), "head", None)
    return jax.shard_map(
        on_device,
        mesh=mesh,
        in_specs=(placed, placed, placed, P("grp")),
        out_specs=placed,
        check_vma=False,
    )
```

```python
import functools
import math

import jax
import jax.numpy as jnp
from jax import lax
from jax.experimental import pallas as pl
from jax.experimental.pallas import tpu as pltpu
from jax.sharding import PartitionSpec as P

MESH = pl.DeviceIdType.MESH
NEG = -1e30


def gather_attend(
    n,
    heads,
    groups,
    tile,
    table_hbm,
    q_hbm,
    k_hbm,
    v_hbm,
    out_ref,
    table_ref,
    q_ref,
    kv_ref,
    p_ref,
    m_ref,
    l_ref,
    acc_ref,
    load_sem,
    send_sem,
    recv_sem,
):
    me = lax.axis_index("seq")
    rows, width = q_ref.shape
    tokens = rows // heads
    half = tokens // 2
    per_group = heads // groups
    cols = tokens * groups
    piece = cols // 2
    factor_scale = width ** (-0.5) * math.log2(math.e)
    right, left = me + 1, me - 1
    has_right, has_left = me < n - 1, me > 0
    barrier = pltpu.get_barrier_semaphore()

    @pl.when(has_right)
    def _():
        pl.semaphore_signal(barrier, inc=1, device_id={"seq": right}, device_id_type=MESH)

    @pl.when(has_left)
    def _():
        pl.semaphore_signal(barrier, inc=1, device_id={"seq": left}, device_id_type=MESH)

    loads = [
        pltpu.make_async_copy(k_hbm, kv_ref.at[me, 0], load_sem.at[0]),
        pltpu.make_async_copy(v_hbm, kv_ref.at[me, 1], load_sem.at[1]),
        pltpu.make_async_copy(table_hbm, table_ref, load_sem.at[2]),
        pltpu.make_async_copy(q_hbm, q_ref, load_sem.at[3]),
    ]
    for load in loads:
        load.start()

    pl.semaphore_wait(barrier, has_right.astype(jnp.int32) + has_left.astype(jnp.int32))

    def remote(shard, which, way):
        part = kv_ref.at[shard, which // 2, pl.ds((which % 2) * piece, piece)]
        return pltpu.make_async_remote_copy(
            src_ref=part,
            dst_ref=part,
            send_sem=send_sem.at[way, shard, which],
            recv_sem=recv_sem.at[shard, which],
            device_id={"seq": left if way else right},
            device_id_type=MESH,
        )

    for which in range(4):
        if which % 2 == 0:
            loads[which // 2].wait()

        @pl.when(has_right)
        def _():
            remote(me, which, 0).start()

        @pl.when(has_left)
        def _():
            remote(me, which, 1).start()

    m_ref[...] = jnp.full(m_ref.shape, NEG, jnp.float32)
    l_ref[...] = jnp.zeros(l_ref.shape, jnp.float32)
    acc_ref[...] = jnp.zeros(acc_ref.shape, jnp.float32)
    loads[2].wait()
    loads[3].wait()

    lane = lax.broadcasted_iota(jnp.int32, (heads, cols), 1)
    head = lax.broadcasted_iota(jnp.int32, (heads, cols), 0)
    matched = lane % groups == head // per_group
    key_token = lane // groups

    def take(distance, which):
        from_left, from_right = me - distance, me + distance

        @pl.when(from_left >= 0)
        def _():
            remote(from_left, which, 0).wait_recv()

            @pl.when(has_right)
            def _():
                remote(from_left, which, 0).start()

        @pl.when(from_right < n)
        def _():
            remote(from_right, which, 1).wait_recv()

            @pl.when(has_left)
            def _():
                remote(from_right, which, 1).start()

    def scores(shard, section, start):
        span = pl.ds(pl.multiple_of((section * half + start) * heads, tile * heads), tile * heads)
        first, second = table_ref[2 * shard], table_ref[2 * shard + 1]
        key_pos = jnp.where(
            key_token < half, first * half + key_token, (second - 1) * half + key_token
        )
        key_code = jnp.where(matched, key_pos, 2**30)
        offset = table_ref[2 * me + section] * half + start
        raw = lax.dot_general(
            q_ref[span, :],
            kv_ref[shard, 0],
            (((1,), (1,)), ((), ())),
            preferred_element_type=jnp.float32,
        )
        shaped = raw.reshape(tile, heads, cols)
        query_pos = lax.broadcasted_iota(jnp.int32, shaped.shape, 0) + offset
        shaped = jnp.where(key_code[None] <= query_pos, shaped, NEG)
        raw = shaped.reshape(tile * heads, cols)
        old_max = m_ref[span, :]
        new_max = jnp.maximum(old_max, jnp.max(raw, axis=-1, keepdims=True))
        fade = jnp.exp2((old_max - new_max) * factor_scale)
        total = l_ref[span, :] * fade
        pieces = []
        for low in range(0, cols, width):
            weights = jnp.exp2((raw[:, low : low + width] - new_max) * factor_scale)
            total += weights
            pieces.append(weights.astype(p_ref.dtype))
        m_ref[span, :] = new_max
        l_ref[span, :] = total
        return span, jnp.concatenate(pieces, axis=1), fade

    def both(shard, section):
        for start in range(0, half, tile):
            span, weights, fade = scores(shard, section, start)
            acc_ref[span, :] = acc_ref[span, :] * fade + jnp.dot(
                weights, kv_ref[shard, 1], preferred_element_type=jnp.float32
            )

    def own(section, carry):
        both(me, section)
        return carry

    lax.fori_loop(0, 2, own, 0)

    def catch_up(distance, section):
        def side(way, carry):
            shard = jnp.where(way == 0, me - distance, me + distance)

            @pl.when((distance > 0) & (shard >= 0) & (shard < n))
            def _():
                both(shard, section)

            return carry

        lax.fori_loop(0, 2, side, 0)

    def round_of(distance, carry):
        def section_of(section, carry):
            take(distance, section)
            catch_up(distance - 1, section)
            return carry

        lax.fori_loop(0, 2, section_of, 0)

        @pl.when((distance < n - 1) | (has_left & has_right))
        def _():
            for which in (2, 3):
                take(distance, which)

        return carry

    lax.fori_loop(1, n, round_of, 0)

    at_end = jnp.logical_not(has_left & has_right)
    if n > 1:

        @pl.when(at_end)
        def _():
            last = n - 1 - me
            for section in range(2):
                for start in range(0, half, tile):
                    span, weights, fade = scores(last, section, start)
                    p_ref[span, :] = weights
                    acc_ref[span, :] = acc_ref[span, :] * fade
            for which in (2, 3):
                take(n - 1, which)
            for start in range(0, tokens, tile):
                span = pl.ds(start * heads, tile * heads)
                acc_ref[span, :] += jnp.dot(
                    p_ref[span, :], kv_ref[last, 1], preferred_element_type=jnp.float32
                )

    for start in range(0, tokens, tile):
        span = pl.ds(start * heads, tile * heads)
        total = jnp.sum(l_ref[span, :], axis=-1, keepdims=True)
        out_ref[span, :] = (acc_ref[span, :] / total).astype(out_ref.dtype)

    def settle(distance, carry):
        for which in range(4):

            @pl.when((me - distance >= 0) & has_right)
            def _():
                remote(me - distance, which, 0).wait_send()

            @pl.when((me + distance < n) & has_left)
            def _():
                remote(me + distance, which, 1).wait_send()

        return carry

    lax.fori_loop(0, n, settle, 0)


def on_device(queries, keys, values, block_order):
    n = lax.axis_size("seq")
    tokens, heads, width = queries.shape
    groups = keys.shape[1]
    rows, cols = tokens * heads, tokens * groups
    tile = min(32, tokens // 2)
    anywhere = pl.BlockSpec(memory_space=pltpu.HBM)
    out = pl.pallas_call(
        functools.partial(gather_attend, n, heads, groups, tile),
        out_shape=pltpu.VMEM((rows, width), queries.dtype),
        in_specs=[anywhere] * 4,
        out_specs=pl.BlockSpec(memory_space=pltpu.VMEM),
        scratch_shapes=[
            pltpu.SMEM(block_order.shape, block_order.dtype),
            pltpu.VMEM((rows, width), queries.dtype),
            pltpu.VMEM((n, 2, cols, width), keys.dtype),
            pltpu.VMEM((rows, cols), values.dtype),
            pltpu.VMEM((rows, width), jnp.float32),
            pltpu.VMEM((rows, width), jnp.float32),
            pltpu.VMEM((rows, width), jnp.float32),
            pltpu.SemaphoreType.DMA((4,)),
            pltpu.SemaphoreType.DMA((2, n, 4)),
            pltpu.SemaphoreType.DMA((n, 4)),
        ],
        compiler_params=pltpu.CompilerParams(collective_id=0, has_side_effects=True),
    )(
        block_order,
        queries.reshape(rows, width),
        keys.reshape(cols, width),
        values.reshape(cols, width),
    )
    return out.reshape(tokens, heads, width)


def solution(mesh):
    placed = P(("grp", "seq"), "head", None)
    return jax.shard_map(
        on_device,
        mesh=mesh,
        in_specs=(placed, placed, placed, P("grp")),
        out_specs=placed,
        check_vma=False,
    )
```

```python
import functools
import math

import jax
import jax.numpy as jnp
from jax import lax
from jax.experimental import pallas as pl
from jax.experimental.pallas import tpu as pltpu
from jax.sharding import PartitionSpec as P

MESH = pl.DeviceIdType.MESH
NEG = -1e30


def gather_attend(
    n,
    heads,
    groups,
    tile,
    table_hbm,
    q_hbm,
    k_hbm,
    v_hbm,
    out_ref,
    table_ref,
    q_ref,
    kv_ref,
    p_ref,
    m_ref,
    l_ref,
    acc_ref,
    load_sem,
    send_sem,
    recv_sem,
):
    me = lax.axis_index("seq")
    rows, width = q_ref.shape
    tokens = rows // heads
    half = tokens // 2
    per_group = heads // groups
    cols = tokens * groups
    piece = cols // 2
    factor_scale = width ** (-0.5) * math.log2(math.e)
    right, left = me + 1, me - 1
    has_right, has_left = me < n - 1, me > 0
    early = True
    barrier = pltpu.get_barrier_semaphore()

    @pl.when(has_right)
    def _():
        pl.semaphore_signal(barrier, inc=1, device_id={"seq": right}, device_id_type=MESH)

    @pl.when(has_left)
    def _():
        pl.semaphore_signal(barrier, inc=1, device_id={"seq": left}, device_id_type=MESH)

    loads = [
        pltpu.make_async_copy(k_hbm, kv_ref.at[me, 0], load_sem.at[0]),
        pltpu.make_async_copy(v_hbm, kv_ref.at[me, 1], load_sem.at[1]),
        pltpu.make_async_copy(table_hbm, table_ref, load_sem.at[2]),
        pltpu.make_async_copy(q_hbm, q_ref, load_sem.at[3]),
    ]
    for load in loads:
        load.start()

    pl.semaphore_wait(barrier, has_right.astype(jnp.int32) + has_left.astype(jnp.int32))

    def remote(shard, which, way):
        part = kv_ref.at[shard, which // 2, pl.ds((which % 2) * piece, piece)]
        return pltpu.make_async_remote_copy(
            src_ref=part,
            dst_ref=part,
            send_sem=send_sem.at[way, shard, which],
            recv_sem=recv_sem.at[shard, which],
            device_id={"seq": left if way else right},
            device_id_type=MESH,
        )

    for which in range(4):
        if which % 2 == 0:
            loads[which // 2].wait()

        @pl.when(has_right)
        def _():
            remote(me, which, 0).start()

        @pl.when(has_left)
        def _():
            remote(me, which, 1).start()

    m_ref[...] = jnp.full(m_ref.shape, NEG, jnp.float32)
    l_ref[...] = jnp.zeros(l_ref.shape, jnp.float32)
    acc_ref[...] = jnp.zeros(acc_ref.shape, jnp.float32)
    loads[2].wait()
    loads[3].wait()

    lane = lax.broadcasted_iota(jnp.int32, (heads, cols), 1)
    head = lax.broadcasted_iota(jnp.int32, (heads, cols), 0)
    matched = lane % groups == head // per_group
    key_token = lane // groups

    def take(distance, which):
        from_left, from_right = me - distance, me + distance

        @pl.when(from_left >= 0)
        def _():
            remote(from_left, which, 0).wait_recv()

            @pl.when(has_right)
            def _():
                remote(from_left, which, 0).start()

        @pl.when(from_right < n)
        def _():
            remote(from_right, which, 1).wait_recv()

            @pl.when(has_left)
            def _():
                remote(from_right, which, 1).start()

    def scores(shard, section, start):
        span = pl.ds(pl.multiple_of((section * half + start) * heads, tile * heads), tile * heads)
        first, second = table_ref[2 * shard], table_ref[2 * shard + 1]
        key_pos = jnp.where(
            key_token < half, first * half + key_token, (second - 1) * half + key_token
        )
        key_code = jnp.where(matched, key_pos, 2**30)
        offset = table_ref[2 * me + section] * half + start
        raw = lax.dot_general(
            q_ref[span, :],
            kv_ref[shard, 0],
            (((1,), (1,)), ((), ())),
            preferred_element_type=jnp.float32,
        )
        shaped = raw.reshape(tile, heads, cols)
        query_pos = lax.broadcasted_iota(jnp.int32, shaped.shape, 0) + offset
        shaped = jnp.where(key_code[None] <= query_pos, shaped, NEG)
        raw = shaped.reshape(tile * heads, cols)
        old_max = m_ref[span, :]
        new_max = jnp.maximum(old_max, jnp.max(raw, axis=-1, keepdims=True))
        fade = jnp.exp2((old_max - new_max) * factor_scale)
        total = l_ref[span, :] * fade
        pieces = []
        for low in range(0, cols, width):
            weights = jnp.exp2((raw[:, low : low + width] - new_max) * factor_scale)
            total += weights
            pieces.append(weights.astype(p_ref.dtype))
        m_ref[span, :] = new_max
        l_ref[span, :] = total
        return span, jnp.concatenate(pieces, axis=1), fade

    def both(shard, section, start):
        span, weights, fade = scores(shard, section, start)
        acc_ref[span, :] = acc_ref[span, :] * fade + jnp.dot(
            weights, kv_ref[shard, 1], preferred_element_type=jnp.float32
        )

    def whole(shard):
        def section_of(section, carry):
            for start in range(0, half, tile):
                both(shard, section, start)
            return carry

        lax.fori_loop(0, 2, section_of, 0)

    whole(me)

    def at(index, way):
        return jnp.where(way == 0, me - index, me + index)

    def relay_round(distance, carry):
        def side(way):
            shard = at(distance - 1, way)

            @pl.when((distance > 1) & (shard >= 0) & (shard < n))
            def _():
                whole(shard)

        if early:
            side(0)
        for which in range(4):
            take(distance, which)
        if not early:
            side(0)
        side(1)
        return carry

    def end_round(distance, carry):
        shard = jnp.where(has_left, me - distance, me + distance)
        for which in range(4):
            take(distance, which)
        whole(shard)
        return carry

    def settle(distance, carry):
        for which in range(4):

            @pl.when((me - distance >= 0) & has_right)
            def _():
                remote(me - distance, which, 0).wait_send()

            @pl.when((me + distance < n) & has_left)
            def _():
                remote(me + distance, which, 1).wait_send()

        return carry

    def close():
        for start in range(0, tokens, tile):
            span = pl.ds(start * heads, tile * heads)
            scale = 1.0 / jnp.sum(l_ref[span, :], axis=-1, keepdims=True)
            out_ref[span, :] = (acc_ref[span, :] * scale).astype(out_ref.dtype)

    if n == 1:
        close()
        return

    interior = has_left & has_right

    @pl.when(interior)
    def _():
        lax.fori_loop(1, n - 1, relay_round, 0)
        lax.fori_loop(0, n - 2, settle, 0)
        relay_round(n - 1, 0)
        close()
        settle(n - 2, 0)

    @pl.when(jnp.logical_not(interior))
    def _():
        lax.fori_loop(1, n - 1, end_round, 0)
        settle(0, 0)
        last = n - 1 - me
        for which in (0, 1):
            take(n - 1, which)
        for start in range(0, tokens, tile):
            span, weights, fade = scores(last, start // half, start % half)
            scale = 1.0 / jnp.sum(l_ref[span, :], axis=-1, keepdims=True)
            p_ref[span, :] = weights
            acc_ref[span, :] = acc_ref[span, :] * (fade * scale)
            l_ref[span, :] = jnp.broadcast_to(scale, (tile * heads, width))
        for which in (2, 3):
            take(n - 1, which)
        for start in range(0, tokens, tile):
            span = pl.ds(start * heads, tile * heads)
            product = jnp.dot(p_ref[span, :], kv_ref[last, 1], preferred_element_type=jnp.float32)
            out_ref[span, :] = (acc_ref[span, :] + product * l_ref[span, :]).astype(out_ref.dtype)


def on_device(queries, keys, values, block_order):
    n = lax.axis_size("seq")
    tokens, heads, width = queries.shape
    groups = keys.shape[1]
    rows, cols = tokens * heads, tokens * groups
    tile = min(64, tokens // 2)
    anywhere = pl.BlockSpec(memory_space=pltpu.HBM)
    out = pl.pallas_call(
        functools.partial(gather_attend, n, heads, groups, tile),
        out_shape=pltpu.VMEM((rows, width), queries.dtype),
        in_specs=[anywhere] * 4,
        out_specs=pl.BlockSpec(memory_space=pltpu.VMEM),
        scratch_shapes=[
            pltpu.SMEM(block_order.shape, block_order.dtype),
            pltpu.VMEM((rows, width), queries.dtype),
            pltpu.VMEM((n, 2, cols, width), keys.dtype),
            pltpu.VMEM((rows, cols), values.dtype),
            pltpu.VMEM((rows, width), jnp.float32),
            pltpu.VMEM((rows, width), jnp.float32),
            pltpu.VMEM((rows, width), jnp.float32),
            pltpu.SemaphoreType.DMA((4,)),
            pltpu.SemaphoreType.DMA((2, n, 4)),
            pltpu.SemaphoreType.DMA((n, 4)),
        ],
        compiler_params=pltpu.CompilerParams(collective_id=0, has_side_effects=True),
    )(
        block_order,
        queries.reshape(rows, width),
        keys.reshape(cols, width),
        values.reshape(cols, width),
    )
    return out.reshape(tokens, heads, width)


def solution(mesh):
    placed = P(("grp", "seq"), "head", None)
    return jax.shard_map(
        on_device,
        mesh=mesh,
        in_specs=(placed, placed, placed, P("grp")),
        out_specs=placed,
        check_vma=False,
    )
```
